32 devices in a mesh: row: 4 (over z), col: 8 (over y, x, core).
Axes of the slice: x: 2, y: 2, z: 4, core: 2. Of those that a mesh axis runs over, the one named last changes fastest.
Arguments:
- adjacency: int32 [32768, 2048], P('col', 'row'), may hold values from -2147483648 to 2147483647, as said below
- frontier: bfloat16 [65536, 128], P(('row', 'col')), may hold values from 0 to 1, as said below
- visited: int32 [4, 32768], P(None, ('col', 'row')), may hold values from -2147483648 to 2147483647, as said below
Outputs:
- path_counts: float32 [32768, 128], P(('col', 'row'))
- reached_bits: int32 [4, 32768], P(None, ('col', 'row'))
The draws below stay inside these ranges and needn't reach their ends.
Inputs may be any that keep to these rules, and one draw needn't show every extreme that they name: Bit k of adjacency[d, w] is the edge from source vertex 32 w + k to destination d; degrees and edge densities differ between vertices and between blocks of 128 by 128 vertices. `frontier`: values are zero or between 0.1 and 1. Bit k of visited[w, d] tells whether destination d was reached from root 32 w + k.
All inputs are finite; a program needn't handle non-finite values.
Results may differ from the reference program's by a relative error of at most 0.0003.
Values may be sent and summed in bfloat16 or wider, within the bound.
A program may use at most 64 MiB of HBM per device.

```python
import functools
import math
import jax
import jax.numpy as jnp
from jax import lax

SOURCES = 128
NDST = 32768
NSRC = 65536
WORDS = 4


def draw_adjacency(key, part):
    column_words = NSRC // 32
    key_list = jax.random.split(jax.random.fold_in(key, 11), 6)
    vertex_level = jax.random.randint(key_list[0], (NDST, 1), 0, 8, dtype=jnp.int32)
    tile_level = jax.random.randint(key_list[1], (NDST // 128, column_words // 4), 0, 3, dtype=jnp.int32)
    tile_level = jnp.repeat(jnp.repeat(tile_level, 128, axis=0), 4, axis=1)
    rate_base = jnp.int32(2097152 // NSRC)
    threshold = jnp.left_shift(rate_base, vertex_level + tile_level)
    selector = jax.random.randint(key_list[2], (NDST, column_words), 0, 1048576, dtype=jnp.int32)
    packed_words = jax.random.randint(key_list[3], (NDST, column_words), -2147483648, 2147483647, dtype=jnp.int32)
    for section_index in range(2):
        extra_words = jax.random.randint(key_list[4 + section_index], (NDST, column_words), -2147483648, 2147483647, dtype=jnp.int32)
        packed_words = jnp.bitwise_and(packed_words, extra_words)
    return jnp.where(selector < threshold, packed_words, jnp.int32(0))


def draw_frontier(key, part):
    key_list = jax.random.split(jax.random.fold_in(key, 23), 2)
    keep_mask = jax.random.uniform(key_list[0], (NSRC, SOURCES), jnp.float32) < 0.5
    magnitude = 0.1 * jnp.exp(jax.random.uniform(key_list[1], (NSRC, SOURCES), jnp.float32) * math.log(10.0))
    values = jnp.where(keep_mask, magnitude, jnp.float32(0.0))
    return values.astype(jnp.bfloat16)


def draw_visited(key, part):
    key_list = jax.random.split(jax.random.fold_in(key, 37), 2)
    first_words = jax.random.randint(key_list[0], (WORDS, NDST), -2147483648, 2147483647, dtype=jnp.int32)
    second_words = jax.random.randint(key_list[1], (WORDS, NDST), -2147483648, 2147483647, dtype=jnp.int32)
    return jnp.bitwise_and(first_words, second_words)


def setup_inputs(seed: int = 0) -> dict:
    arg_keys = jax.random.split(jax.random.key(seed), 4)
    return {
        "adjacency": draw_adjacency(jax.random.fold_in(arg_keys[3], 71), 0),
        "frontier": draw_frontier(jax.random.fold_in(arg_keys[3], 71), 0),
        "visited": draw_visited(jax.random.fold_in(arg_keys[3], 71), 0),
    }


def expand_bits(packed):
    shift_table = jnp.arange(32, dtype=jnp.int32)
    bit_table = jnp.bitwise_and(jnp.right_shift(packed[:, :, None], shift_table), 1)
    return bit_table.reshape(packed.shape[0], packed.shape[1] * 32).astype(jnp.bfloat16)


def finish(reached, visited):
    row_count = reached.shape[0]
    word_count = visited.shape[0]
    shift_table = jnp.arange(32, dtype=jnp.int32)
    seen_bits = jnp.bitwise_and(jnp.right_shift(visited[:, :, None], shift_table), 1)
    seen_bits = jnp.transpose(seen_bits, (1, 0, 2)).reshape(row_count, word_count * 32)
    path_counts = jnp.where(seen_bits == 1, jnp.float32(0.0), reached)
    fresh = jnp.logical_and(seen_bits == 0, reached > 0).astype(jnp.int32)
    fresh = fresh.reshape(row_count, word_count, 32)
    added = functools.reduce(jnp.bitwise_or, [jnp.left_shift(fresh[:, :, position], position) for position in range(32)])
    reached_bits = jnp.bitwise_or(visited, jnp.transpose(added))
    return path_counts, reached_bits


def reference(adjacency, frontier, visited):
    dst_total = adjacency.shape[0]
    block_len = math.gcd(dst_total, 512)
    blocks = adjacency.reshape(dst_total // block_len, block_len, adjacency.shape[1])

    def one_block(packed):
        return jnp.dot(expand_bits(packed), frontier, preferred_element_type=jnp.float32)

    reached = lax.map(one_block, blocks).reshape(dst_total, frontier.shape[1])
    return finish(reached, visited)
```

```python
import functools
import math

import jax
import jax.numpy as jnp
import numpy as np
from jax import lax
from jax.experimental import pallas as pl
from jax.experimental.pallas import tpu as pltpu
from jax.sharding import PartitionSpec as P

MESH = pl.DeviceIdType.MESH
LOW = 0.09
LEVELS = 65000.0


def expand_bits(words):
    one = jnp.full(words.shape, 1, jnp.float8_e4m3fn)
    zero = jnp.full(words.shape, 0, jnp.float8_e4m3fn)
    pieces = []
    for byte in range(4):
        part = (words >> (8 * byte)).astype(jnp.int8)
        for bit in range(8):
            mask = np.int8(-128) if bit == 7 else np.int8(1 << bit)
            pieces.append(jnp.where((part & mask) != 0, one, zero))
    return jnp.concatenate(pieces, axis=0)


def encode(value, scale):
    code = jnp.log(jnp.maximum(value, LOW)) * scale + (1.5 - math.log(LOW) * scale)
    code = jnp.where(value > 0, code, 0.0).astype(jnp.int32)
    return (code - 32768).astype(jnp.int16)


def decode(code, scale):
    code = code.astype(jnp.int32) + 32768
    value = jnp.exp((code - 1).astype(jnp.float32) * (1.0 / scale) + math.log(LOW))
    return jnp.where(code > 0, value, 0.0)


def flip(index, bit):
    return index + bit - 2 * bit * ((index // bit) % 2)


def kernel(
    n_row, n_col, adj, ft, visited, counts, bits,
    stage, words, fbuf, total, out_code, in_code,
    load_sem, own_sem, fsend, frecv, psend, precv,
):
    r, c = lax.axis_index("row"), lax.axis_index("col")
    dst, width = adj.shape
    depth = ft.shape[1]
    wide = width // n_col
    part = dst // n_row
    half = math.gcd(dst, 2048)
    halves = dst // half
    tile = stage.shape[1]
    tiles = dst // tile
    paired = n_col == 8
    scale = LEVELS / math.log(width * 32 * 1.01 / LOW)

    def load(t, slot):
        return pltpu.make_async_copy(
            adj.at[pl.ds(pl.multiple_of(t * tile, tile), tile), :], stage.at[slot], load_sem.at[slot]
        )

    load(0, 0).start()
    own = pltpu.make_async_copy(ft, fbuf.at[c], own_sem)
    own.start()

    if paired:
        mates = [flip(c, 1), flip(c, 2), flip(c, 4)]
    else:
        mates = [lax.rem(c + i, n_col) for i in range(1, n_col)]
    others = [lax.rem(r + i, n_row) for i in range(1, n_row)]
    barrier = pltpu.get_barrier_semaphore()
    for mate in mates:
        pl.semaphore_signal(barrier, inc=1, device_id={"col": mate}, device_id_type=MESH)
    for other in others:
        pl.semaphore_signal(barrier, inc=1, device_id={"row": other}, device_id_type=MESH)
    pl.semaphore_wait(barrier, len(mates) + len(others))

    def send(src, dst_ref, role, mate):
        return pltpu.make_async_remote_copy(
            src_ref=src, dst_ref=dst_ref, send_sem=fsend.at[role], recv_sem=frecv.at[role],
            device_id={"col": mate}, device_id_type=MESH,
        )

    if paired:
        pair, east, north = mates
        first, second = pl.ds(0, ft.shape[0] // 2), pl.ds(ft.shape[0] // 2, ft.shape[0] // 2)
        diagonal = flip(east, 4)
        slots = [pair, east, north, diagonal, diagonal, flip(pair, 2), flip(pair, 4), flip(diagonal, 1)]
        sends = [
            send(ft, fbuf.at[c], 0, pair),
            send(ft, fbuf.at[c], 1, east),
            send(ft, fbuf.at[c], 2, north),
            send(fbuf.at[east, first], fbuf.at[east, first], 3, north),
            send(fbuf.at[north, second], fbuf.at[north, second], 4, east),
            send(fbuf.at[east], fbuf.at[east], 5, pair),
            send(fbuf.at[north], fbuf.at[north], 6, pair),
            send(fbuf.at[diagonal], fbuf.at[diagonal], 7, pair),
        ]
        for role in (1, 2, 0):
            sends[role].start()

        def arrived(role):
            place = fbuf.at[slots[role]]
            if role == 3:
                place = fbuf.at[diagonal, first]
            if role == 4:
                place = fbuf.at[diagonal, second]
            send(place, place, role, pair).wait_recv()

    else:
        sends = [send(ft, fbuf.at[c], i, mate) for i, mate in enumerate(mates)]
        for copy in sends:
            copy.start()

    @pl.loop(0, tiles)
    def _(t):
        slot = lax.rem(t, 2)

        @pl.when(t + 1 < tiles)
        def _():
            load(t + 1, 1 - slot).start()

        load(t, slot).wait()
        words[:, pl.ds(pl.multiple_of(t * tile, tile), tile)] = stage[slot].T

    total[...] = jnp.zeros_like(total)
    own.wait()

    def product(slot, start, size):
        packed = words[pl.ds(pl.multiple_of(slot * wide, wide), wide), pl.ds(start, size)]
        return lax.dot_general(
            fbuf[slot], expand_bits(packed), (((1,), (0,)), ((), ())), preferred_element_type=jnp.float32
        )

    early = n_col - 2

    @pl.loop(0, early * halves)
    def _(t):
        step = t // halves
        start = pl.multiple_of(lax.rem(t, halves) * half, half)
        fresh = lax.rem(t, halves) == 0
        if paired:

            @pl.when(jnp.logical_and(fresh, step == 1))
            def _():
                arrived(0)

            @pl.when(jnp.logical_and(fresh, step == 2))
            def _():
                arrived(1)
                sends[3].start()
                sends[5].start()
                arrived(2)
                sends[4].start()
                sends[6].start()

            @pl.when(jnp.logical_and(fresh, step == 4))
            def _():
                arrived(5)

            @pl.when(jnp.logical_and(fresh, step == 5))
            def _():
                arrived(6)
                arrived(3)
                arrived(4)
                sends[7].start()

            slot = c
            for number, choice in enumerate((slots[0], slots[1], slots[2], slots[5], slots[6])):
                slot = jnp.where(step == number + 1, choice, slot)
        else:
            slot = lax.rem(c + n_col - step, n_col)

            @pl.when(jnp.logical_and(fresh, step > 0))
            def _():
                send(fbuf.at[slot], fbuf.at[slot], step - 1, mates[0]).wait_recv()

        total[:, pl.ds(start, half)] += product(slot, start, half)

    if paired:
        arrived(7)
        last = (slots[3], slots[7])
    else:
        last = (lax.rem(c + 2, n_col), lax.rem(c + 1, n_col))
        for slot, role in zip(last, (n_col - 3, n_col - 2)):
            send(fbuf.at[slot], fbuf.at[slot], role, mates[0]).wait_recv()

    def exchange(t, other):
        return pltpu.make_async_remote_copy(
            src_ref=out_code.at[t], dst_ref=in_code.at[t], send_sem=psend.at[t], recv_sem=precv.at[t],
            device_id={"row": other}, device_id_type=MESH,
        )

    @pl.loop(0, n_row)
    def _(t):
        other = lax.rem(r + 1 + t, n_row)
        start = pl.multiple_of(other * part, part)
        block = total[:, pl.ds(start, part)] + product(last[0], start, part)
        block = block + product(last[1], start, part)

        @pl.when(t < n_row - 1)
        def _():
            out_code[t] = encode(block, scale)
            exchange(t, other).start()

        @pl.when(t == n_row - 1)
        def _():
            total[:, pl.ds(0, part)] = block

    def received(t, value):
        exchange(t, others[0]).wait_recv()
        return value + decode(in_code[t], scale)

    reached = total[:, pl.ds(0, part)]
    for t in range(n_row - 1):
        reached = received(t, reached)
    place = lax.broadcasted_iota(jnp.int32, (32, part), 0)
    kept, added = [], []
    for word in range(visited.shape[0]):
        value = reached[word * 32 : word * 32 + 32]
        unseen = ((visited[word : word + 1, :] >> place) & 1) == 0
        kept.append(jnp.where(unseen, value, 0.0))
        marks = jnp.where(jnp.logical_and(unseen, value > 0), jnp.int32(1) << place, 0)
        added.append(jnp.sum(marks, axis=0, keepdims=True))
    counts[...] = jnp.concatenate(kept, axis=0).T
    bits[...] = visited[...] | jnp.concatenate(added, axis=0)
    for copy in sends:
        copy.wait_send()
    for t in range(n_row - 1):
        exchange(t, others[0]).wait_send()


def shards(n_row, n_col, adjacency, frontier, visited):
    dst, width = adjacency.shape
    depth, roots = frontier.shape
    part = dst // n_row
    tile = math.gcd(dst, 256)
    ft = jnp.transpose(frontier.reshape(depth // 32, 32, roots), (2, 1, 0)).reshape(roots, depth)
    vmem = pl.BlockSpec(memory_space=pltpu.VMEM)
    roles = 8 if n_col == 8 else n_col - 1
    dma = pltpu.SemaphoreType.DMA
    return pl.pallas_call(
        functools.partial(kernel, n_row, n_col),
        out_shape=(
            jax.ShapeDtypeStruct((part, roots), jnp.float32),
            jax.ShapeDtypeStruct((visited.shape[0], part), jnp.int32),
        ),
        in_specs=[pl.BlockSpec(memory_space=pl.ANY), vmem, vmem],
        out_specs=(vmem, vmem),
        scratch_shapes=[
            pltpu.VMEM((2, tile, width), jnp.int32),
            pltpu.VMEM((width, dst), jnp.int32),
            pltpu.VMEM((n_col, roots, depth), jnp.bfloat16),
            pltpu.VMEM((roots, dst), jnp.float32),
            pltpu.VMEM((n_row - 1, roots, part), jnp.int16),
            pltpu.VMEM((n_row - 1, roots, part), jnp.int16),
            dma((2,)),
            dma,
            dma((roles,)),
            dma((roles,)),
            dma((n_row - 1,)),
            dma((n_row - 1,)),
        ],
        compiler_params=pltpu.CompilerParams(
            collective_id=0, has_side_effects=True, vmem_limit_bytes=56 * 2**20
        ),
    )(adjacency, ft, visited)


def solution(mesh):
    placed = (P("col", "row"), P(("row", "col"), None), P(None, ("col", "row")))
    return jax.shard_map(
        functools.partial(shards, mesh.shape["row"], mesh.shape["col"]),
        mesh=mesh,
        in_specs=placed,
        out_specs=(P(("col", "row"), None), P(None, ("col", "row"))),
        check_vma=False,
    )
```
